256 devices in a mesh: trial: 4 (over y), dp: 32 (over z, x), tp: 2 (over core).
Axes of the slice: x: 4, y: 4, z: 8, core: 2. Of those that a mesh axis runs over, the one named last changes fastest.
Arguments:
- slope_query: float32 [128, 768, 768], P(('trial', 'dp'), None, 'tp'), parts along dimension 0, may hold values from -6 to 6
- slope_key: float32 [128, 768, 768], P(('trial', 'dp'), None, 'tp'), parts along dimension 0, may hold values from -6 to 6
- slope_value: float32 [128, 768, 768], P(('trial', 'dp'), None, 'tp'), parts along dimension 0, may hold values from -6 to 6
- slope_mixed: float32 [128, 768, 768], P(('trial', 'dp'), 'tp'), parts along dimension 0, may hold values from -6 to 6
- slope_norm: float32 [128, 768], P(('trial', 'dp')), parts along dimension 0, may hold values from -12 to 12
- slope_bias: float32 [128, 768], P(('trial', 'dp')), parts along dimension 0, may hold values from -12 to 12
- param_query: float32 [3072, 768], P(('trial', 'dp'), 'tp'), parts along dimension 0, may hold values from -0.4375 to 0.4375
- param_key: float32 [3072, 768], P(('trial', 'dp'), 'tp'), parts along dimension 0, may hold values from -0.4375 to 0.4375
- param_value: float32 [3072, 768], P(('trial', 'dp'), 'tp'), parts along dimension 0, may hold values from -0.4375 to 0.4375
- param_mixed: float32 [3072, 768], P(('trial', 'tp'), 'dp'), parts along dimension 0, may hold values from -0.4375 to 0.4375
- param_norm: float32 [3072], P(('trial', 'dp')), parts along dimension 0, may hold values from 0.25 to 1.75
- param_bias: float32 [3072], P(('trial', 'dp')), parts along dimension 0, may hold values from -3 to 3
- state_query: float32 [3072, 768], P(('trial', 'dp'), 'tp'), parts along dimension 0, may hold values from 0.00026041668 to 0.0026041667
- state_key: float32 [3072, 768], P(('trial', 'dp'), 'tp'), parts along dimension 0, may hold values from 0.00026041668 to 0.0026041667
- state_value: float32 [3072, 768], P(('trial', 'dp'), 'tp'), parts along dimension 0, may hold values from 0.00026041668 to 0.0026041667
- state_mixed: float32 [3072, 768], P(('trial', 'tp'), 'dp'), parts along dimension 0, may hold values from 0.00026041668 to 0.0026041667
- state_norm: float32 [3072], P(('trial', 'dp')), parts along dimension 0, may hold values from 0.05 to 0.8
- state_bias: float32 [3072], P(('trial', 'dp')), parts along dimension 0, may hold values from 0.05 to 0.8
Outputs:
- half_query: bfloat16 [3072, 768], P('trial', 'tp'), parts along dimension 0
- half_key: bfloat16 [3072, 768], P('trial', 'tp'), parts along dimension 0
- half_value: bfloat16 [3072, 768], P('trial', 'tp'), parts along dimension 0
- half_mixed: bfloat16 [3072, 768], P(('trial', 'tp')), parts along dimension 0
- half_norm: bfloat16 [3072], P('trial'), parts along dimension 0
- half_bias: bfloat16 [3072], P('trial'), parts along dimension 0
- next_query: float32 [3072, 768], P(('trial', 'dp'), 'tp'), parts along dimension 0
- next_key: float32 [3072, 768], P(('trial', 'dp'), 'tp'), parts along dimension 0
- next_value: float32 [3072, 768], P(('trial', 'dp'), 'tp'), parts along dimension 0
- next_mixed: float32 [3072, 768], P(('trial', 'tp'), 'dp'), parts along dimension 0
- next_norm: float32 [3072], P(('trial', 'dp')), parts along dimension 0
- next_bias: float32 [3072], P(('trial', 'dp')), parts along dimension 0
- state_new_query: float32 [3072, 768], P(('trial', 'dp'), 'tp'), parts along dimension 0
- state_new_key: float32 [3072, 768], P(('trial', 'dp'), 'tp'), parts along dimension 0
- state_new_value: float32 [3072, 768], P(('trial', 'dp'), 'tp'), parts along dimension 0
- state_new_mixed: float32 [3072, 768], P(('trial', 'tp'), 'dp'), parts along dimension 0
- state_new_norm: float32 [3072], P(('trial', 'dp')), parts along dimension 0
- state_new_bias: float32 [3072], P(('trial', 'dp')), parts along dimension 0
The draws below stay inside these ranges and needn't reach their ends.
There are 4 independent parts, one for each index of `trial`. The reference program is written for one: setup_inputs(seed, part) draws one part's arguments, and reference() takes and returns one part's arrays. A program takes and returns all parts, laid end to end along the dimension named above; each array names one. Nothing has to cross between parts.
All inputs are finite; a program needn't handle non-finite values.
Results may differ from the reference program's by a relative error of at most 0.001.
Values may be sent and summed in bfloat16 or wider, within the bound.
No kernel may reach another device: no remote copies, remote signals or barrier semaphores. Data moves between devices by JAX's collectives and lax.ppermute only.
A program may use at most 64 MiB of HBM per device.

```python
import jax
import jax.numpy as jnp
from jax import lax

WIDTH = 768
ATTN = 768
REPLICAS = 32


def with_spikes(entries, rng, source, target, parts, factor):
    owner, partner = [(jnp.arange(entries.shape[position]) // (entries.shape[position] // parts)).reshape([-1 if axis == position else 1 for axis in range(entries.ndim)]) for position in (source, target)]
    chosen = jax.random.permutation(rng, parts)[partner]
    strong = (owner == chosen) | (owner == (partner + parts // 2) % parts)
    return jnp.where(strong, factor * entries, entries)


def steps_of(stream_key, shape, split, low, top_value):
    gain = 1.0
    for axis_at, blocks in split:
        steps = jax.random.uniform(jax.random.fold_in(jax.random.fold_in(stream_key, 6), axis_at), (blocks,), jnp.float32, low / len(split), top_value / len(split))
        gain = gain * jnp.repeat(jnp.exp(steps), shape[axis_at] // blocks).reshape((-1,) + (1,) * (len(shape) - 1 - axis_at))
    return gain


def gaussian(rng, extent, scale, most, cuts=(), dtype=jnp.bfloat16):
    factor_of = steps_of(rng, extent, cuts, -0.22, 0.18) if cuts else 1.0
    result = jax.random.normal(rng, extent, jnp.float32) * scale * factor_of
    return jnp.minimum(jnp.maximum(result, -most), most).astype(dtype)


def gaussian_with(key, dims, width, most, shards, heavy, held_as=jnp.bfloat16):
    values = width * jax.random.normal(key, dims, jnp.float32)
    if shards:
        values = values * steps_of(key, dims, shards, -0.22, 0.18)
    return jnp.clip(with_spikes(values, jax.random.fold_in(key, 3), *heavy), -most, most).astype(held_as)


def setup_inputs(seed: int = 0, part: int = 0) -> dict:
    streams_of = jax.random.split(jax.random.key(seed), 19)
    part_splits = jax.random.split(jax.random.fold_in(streams_of[18], part), 19)
    return {
        "slope_query": gaussian_with(part_splits[0], (REPLICAS, WIDTH, ATTN), 0.5, 6.0, ((0, 32), (2, 2)), (0, 1, 32, 2.75), jnp.float32),
        "slope_key": gaussian_with(part_splits[1], (REPLICAS, WIDTH, ATTN), 0.5, 6.0, ((0, 32), (2, 2)), (0, 1, 32, 2.75), jnp.float32),
        "slope_value": gaussian_with(part_splits[2], (REPLICAS, WIDTH, ATTN), 0.5, 6.0, ((0, 32), (2, 2)), (0, 1, 32, 2.75), jnp.float32),
        "slope_mixed": gaussian_with(part_splits[3], (REPLICAS, ATTN, WIDTH), 0.5, 6.0, ((0, 32), (1, 2)), (0, 2, 32, 2.75), jnp.float32),
        "slope_norm": gaussian_with(part_splits[4], (REPLICAS, WIDTH), 1.0, 12.0, ((0, 32),), (0, 1, 32, 2.75), jnp.float32),
        "slope_bias": gaussian_with(part_splits[5], (REPLICAS, WIDTH), 1.0, 12.0, ((0, 32),), (0, 1, 32, 2.75), jnp.float32),
        "param_query": gaussian_with(part_splits[6], (WIDTH, ATTN), WIDTH ** -0.5, 0.4375, ((0, 32), (1, 2)), (1, 0, 32, 2.75), jnp.float32),
        "param_key": gaussian_with(part_splits[7], (WIDTH, ATTN), WIDTH ** -0.5, 0.4375, ((0, 32), (1, 2)), (1, 0, 32, 2.75), jnp.float32),
        "param_value": gaussian_with(part_splits[8], (WIDTH, ATTN), WIDTH ** -0.5, 0.4375, ((0, 32), (1, 2)), (1, 0, 32, 2.75), jnp.float32),
        "param_mixed": gaussian_with(part_splits[9], (ATTN, WIDTH), ATTN ** -0.5, 0.4375, ((0, 2), (1, 32)), (0, 1, 32, 2.75), jnp.float32),
        "param_norm": jnp.clip(1.0 + 0.15 * jax.random.normal(part_splits[10], (WIDTH,), jnp.float32), 0.25, 1.75),
        "param_bias": gaussian(part_splits[11], (WIDTH,), 0.5, 3.0, ((0, 32),), jnp.float32),
        "state_query": jnp.clip(0.00026041668 + 0.00234375 * jax.random.uniform(part_splits[12], (WIDTH, ATTN), jnp.float32) ** steps_of(part_splits[12], (WIDTH, ATTN), ((0, 32), (1, 2)), -0.2, 0.2), 0.00026041668, 0.0026041667),
        "state_key": jnp.clip(0.00026041668 + 0.00234375 * jax.random.uniform(part_splits[13], (WIDTH, ATTN), jnp.float32) ** steps_of(part_splits[13], (WIDTH, ATTN), ((0, 32), (1, 2)), -0.2, 0.2), 0.00026041668, 0.0026041667),
        "state_value": jnp.clip(0.00026041668 + 0.00234375 * jax.random.uniform(part_splits[14], (WIDTH, ATTN), jnp.float32) ** steps_of(part_splits[14], (WIDTH, ATTN), ((0, 32), (1, 2)), -0.2, 0.2), 0.00026041668, 0.0026041667),
        "state_mixed": jnp.clip(0.00026041668 + 0.00234375 * jax.random.uniform(part_splits[15], (ATTN, WIDTH), jnp.float32) ** steps_of(part_splits[15], (ATTN, WIDTH), ((0, 2), (1, 32)), -0.2, 0.2), 0.00026041668, 0.0026041667),
        "state_norm": jnp.clip(0.05 + 0.75 * jax.random.uniform(part_splits[16], (WIDTH,), jnp.float32) ** steps_of(part_splits[16], (WIDTH,), ((0, 32),), -0.2, 0.2), 0.05, 0.8),
        "state_bias": jnp.clip(0.05 + 0.75 * jax.random.uniform(part_splits[17], (WIDTH,), jnp.float32) ** steps_of(part_splits[17], (WIDTH,), ((0, 32),), -0.2, 0.2), 0.05, 0.8),
    }


learn_rate = 0.02
hold_rate = 0.8

def reference(slope_query, slope_key, slope_value, slope_mixed, slope_norm, slope_bias, param_query, param_key, param_value, param_mixed, param_norm, param_bias, state_query, state_key, state_value, state_mixed, state_norm, state_bias):
    mean_query = lax.optimization_barrier(jnp.sum(slope_query.astype(jnp.float32), axis=0)) * REPLICAS ** (-0.5)
    mean_key = lax.optimization_barrier(jnp.sum(slope_key.astype(jnp.float32), axis=0)) * REPLICAS ** (-0.5)
    mean_value = lax.optimization_barrier(jnp.sum(slope_value.astype(jnp.float32), axis=0)) * REPLICAS ** (-0.5)
    mean_mixed = lax.optimization_barrier(jnp.sum(slope_mixed.astype(jnp.float32), axis=0)) * REPLICAS ** (-0.5)
    mean_norm = lax.optimization_barrier(jnp.sum(slope_norm.astype(jnp.float32), axis=0)) * REPLICAS ** (-0.5)
    mean_bias = lax.optimization_barrier(jnp.sum(slope_bias.astype(jnp.float32), axis=0)) * REPLICAS ** (-0.5)
    ratio_query = jnp.sqrt(lax.optimization_barrier(jnp.sum(param_query * param_query, axis=1, keepdims=True))) * lax.rsqrt(lax.optimization_barrier(jnp.sum(mean_query * mean_query, axis=1, keepdims=True)) + 1e-06)
    mean_query = mean_query * ratio_query
    ratio_key = jnp.sqrt(lax.optimization_barrier(jnp.sum(param_key * param_key, axis=1, keepdims=True))) * lax.rsqrt(lax.optimization_barrier(jnp.sum(mean_key * mean_key, axis=1, keepdims=True)) + 1e-06)
    mean_key = mean_key * ratio_key
    ratio_value = jnp.sqrt(lax.optimization_barrier(jnp.sum(param_value * param_value, axis=1, keepdims=True))) * lax.rsqrt(lax.optimization_barrier(jnp.sum(mean_value * mean_value, axis=1, keepdims=True)) + 1e-06)
    mean_value = mean_value * ratio_value
    ratio_mixed = jnp.sqrt(lax.optimization_barrier(jnp.sum(param_mixed * param_mixed, axis=0, keepdims=True))) * lax.rsqrt(lax.optimization_barrier(jnp.sum(mean_mixed * mean_mixed, axis=0, keepdims=True)) + 1e-06)
    mean_mixed = mean_mixed * ratio_mixed
    state_new_query = hold_rate * state_query + (1.0 - hold_rate) * mean_query * mean_query
    next_query = param_query - learn_rate * mean_query * lax.rsqrt(state_new_query + 1e-06)
    state_new_key = hold_rate * state_key + (1.0 - hold_rate) * mean_key * mean_key
    next_key = param_key - learn_rate * mean_key * lax.rsqrt(state_new_key + 1e-06)
    state_new_value = hold_rate * state_value + (1.0 - hold_rate) * mean_value * mean_value
    next_value = param_value - learn_rate * mean_value * lax.rsqrt(state_new_value + 1e-06)
    state_new_mixed = hold_rate * state_mixed + (1.0 - hold_rate) * mean_mixed * mean_mixed
    next_mixed = param_mixed - learn_rate * mean_mixed * lax.rsqrt(state_new_mixed + 1e-06)
    state_new_norm = hold_rate * state_norm + (1.0 - hold_rate) * mean_norm * mean_norm
    next_norm = param_norm - learn_rate * mean_norm * lax.rsqrt(state_new_norm + 1e-06)
    state_new_bias = hold_rate * state_bias + (1.0 - hold_rate) * mean_bias * mean_bias
    next_bias = param_bias - learn_rate * mean_bias * lax.rsqrt(state_new_bias + 1e-06)
    half_query = next_query.astype(jnp.bfloat16)
    half_key = next_key.astype(jnp.bfloat16)
    half_value = next_value.astype(jnp.bfloat16)
    half_mixed = next_mixed.astype(jnp.bfloat16)
    half_norm = next_norm.astype(jnp.bfloat16)
    half_bias = next_bias.astype(jnp.bfloat16)
    return (half_query, half_key, half_value, half_mixed, half_norm, half_bias, next_query, next_key, next_value, next_mixed, next_norm, next_bias, state_new_query, state_new_key, state_new_value, state_new_mixed, state_new_norm, state_new_bias)
```

```python
import jax
import jax.numpy as jnp
from jax import lax
from jax.sharding import Mesh
from jax.sharding import PartitionSpec as P

learn_rate = 0.02
hold_rate = 0.8


def shift(a, axis, by):
    n = lax.axis_size(axis)
    return lax.ppermute(a, axis, [(i, (i + by) % n) for i in range(n)])


def ring_sum(pick, axis, half):
    n = lax.axis_size(axis)
    far = pick(n // 2)
    up = shift(far[:half], axis, 1)
    down = shift(far[half:], axis, -1)
    rest = far.ndim - 1
    tail = far.shape[0] - half
    up = jnp.pad(up, [(0, tail)] + [(0, 0)] * rest)
    down = jnp.pad(down, [(half, 0)] + [(0, 0)] * rest)
    for j in range(n // 2 - 1, 0, -1):
        up = shift(pick(j) + up, axis, 1)
        down = shift(pick(-j) + down, axis, -1)
    return pick(0) + up + down


def direct_sum(pick, axis):
    n = lax.axis_size(axis)
    total = pick(0)
    got = [shift(pick(j), axis, j) for j in range(1, n)]
    for g in got:
        total = total + g
    return total


def direct_gather(own, axis):
    n = lax.axis_size(axis)
    return jnp.stack([own] + [shift(own, axis, j) for j in range(1, n)])


def ring_gather(own, axis, half):
    n = lax.axis_size(axis)
    ups, downs = [own], [own]
    for j in range(1, n // 2):
        ups.append(shift(ups[-1], axis, 1))
        downs.append(shift(downs[-1], axis, -1))
    far = jnp.concatenate([shift(ups[-1][:half], axis, 1), shift(downs[-1][half:], axis, -1)])
    return jnp.stack(ups + [far] + downs[:0:-1])


def in_order(entries, axis, dim):
    n = lax.axis_size(axis)
    at = lax.axis_index(axis)
    flipped = jnp.flip(entries, dim)
    return jnp.roll(flipped, at + 1, dim)


def shards(
    slope_query,
    slope_key,
    slope_value,
    slope_mixed,
    slope_norm,
    slope_bias,
    param_query,
    param_key,
    param_value,
    param_mixed,
    param_norm,
    param_bias,
    state_query,
    state_key,
    state_value,
    state_mixed,
    state_norm,
    state_bias,
):
    nz, nx = lax.axis_size("z"), lax.axis_size("x")
    iz, ix = lax.axis_index("z"), lax.axis_index("x")
    rows, cols = param_query.shape

    small = jnp.stack([slope_norm[0].reshape(nz, nx, rows), slope_bias[0].reshape(nz, nx, rows)], 2)
    small = small.reshape(nz, nx, 1, 2 * rows)
    small = jnp.pad(small, [(0, 0), (0, 0), (0, 7), (0, cols - 2 * rows)])
    first = jnp.concatenate(
        [slope_query.reshape(nz, nx, rows, cols), slope_key.reshape(nz, nx, rows, cols), small], 2
    )
    second = jnp.concatenate(
        [slope_value.reshape(nz, nx, rows, cols), slope_mixed[0].T.reshape(nz, nx, rows, cols)], 2
    )

    def over_x(j):
        return lax.dynamic_index_in_dim(first, (ix + j) % nx, 1, keepdims=False)

    def over_z(j):
        return lax.dynamic_index_in_dim(second, (iz + j) % nz, 0, keepdims=False)

    first = ring_sum(over_x, "x", nz // 2)
    second = ring_sum(over_z, "z", nx // 2)
    first = direct_sum(lambda j: lax.dynamic_index_in_dim(first, (iz + j) % nz, 0, keepdims=False), "z")
    second = direct_sum(lambda j: lax.dynamic_index_in_dim(second, (ix + j) % nx, 0, keepdims=False), "x")

    mean_rate = (nz * nx) ** (-0.5)
    mean = jnp.concatenate([first[: 2 * rows], second]) * mean_rate
    mean_small = first[2 * rows, : 2 * rows] * mean_rate
    param = jnp.concatenate([param_query, param_key, param_value, param_mixed.T])
    state = jnp.concatenate([state_query, state_key, state_value, state_mixed.T])
    param_small = jnp.concatenate([param_norm, param_bias])
    state_small = jnp.concatenate([state_norm, state_bias])

    own = jnp.sum(param * param, axis=1)
    own = own + shift(own, "tp", 1)
    size = jnp.sum(mean * mean, axis=1)
    size = size + shift(size, "tp", 1)
    mean = mean * (jnp.sqrt(own) * lax.rsqrt(size + 1e-06))[:, None]
    state_new = hold_rate * state + (1.0 - hold_rate) * mean * mean
    following = param - learn_rate * mean * lax.rsqrt(state_new + 1e-06)
    state_new_small = hold_rate * state_small + (1.0 - hold_rate) * mean_small * mean_small
    next_small = param_small - learn_rate * mean_small * lax.rsqrt(state_new_small + 1e-06)

    half = following.astype(jnp.bfloat16)
    half_small = jnp.pad(next_small.astype(jnp.bfloat16)[None], [(0, 7), (0, cols - 2 * rows)])
    first = jnp.concatenate([half[: 2 * rows], half_small])
    second = half[2 * rows :]

    first = ring_gather(direct_gather(first, "z"), "x", nz // 2)
    second = ring_gather(direct_gather(second, "x"), "z", nx // 2)
    first = in_order(in_order(first, "x", 0), "z", 1).swapaxes(0, 1)
    second = in_order(in_order(second, "z", 0), "x", 1)

    def whole(a):
        return a.reshape(nz * nx * rows, cols)

    half_small = first[:, :, 2 * rows, : 2 * rows]
    parts = [following[i * rows : (i + 1) * rows] for i in range(4)]
    states = [state_new[i * rows : (i + 1) * rows] for i in range(4)]
    return (
        whole(first[:, :, :rows]),
        whole(first[:, :, rows : 2 * rows]),
        whole(second[:, :, :rows]),
        whole(second[:, :, rows:]).T,
        half_small[:, :, :rows].reshape(-1),
        half_small[:, :, rows:].reshape(-1),
        parts[0],
        parts[1],
        parts[2],
        parts[3].T,
        next_small[:rows],
        next_small[rows:],
        states[0],
        states[1],
        states[2],
        states[3].T,
        state_new_small[:rows],
        state_new_small[rows:],
    )


def solution(mesh):
    trial, dp, tp = (mesh.shape[a] for a in ("trial", "dp", "tp"))
    fine = Mesh(mesh.devices.reshape(trial, dp // 4, 4, tp), ("trial", "z", "x", "tp"))
    rows = P(("trial", "z", "x"), "tp")
    cols = P(("trial", "tp"), ("z", "x"))
    flat = P(("trial", "z", "x"))
    stack = P(("trial", "z", "x"), None, "tp")
    shares = (rows, rows, rows, cols, flat, flat)
    in_specs = (stack, stack, stack, P(("trial", "z", "x"), "tp", None), P(("trial", "z", "x"), None), P(("trial", "z", "x"), None))
    in_specs = in_specs + shares + shares
    out_specs = (P("trial", "tp"),) * 3 + (P(("trial", "tp"), None), P("trial"), P("trial")) + shares + shares
    return jax.shard_map(shards, mesh=fine, in_specs=in_specs, out_specs=out_specs, check_vma=False)
```

```python
import jax
import jax.numpy as jnp
from jax import lax
from jax.sharding import Mesh
from jax.sharding import PartitionSpec as P

learn_rate = 0.02
hold_rate = 0.8


def shift(a, axis, by):
    n = lax.axis_size(axis)
    return lax.ppermute(a, axis, [(i, (i + by) % n) for i in range(n)])


def ring_sum(pick, axis, half):
    n = lax.axis_size(axis)
    far = pick(n // 2)
    up = shift(far[:half], axis, 1)
    down = shift(far[half:], axis, -1)
    rest = far.ndim - 1
    tail = far.shape[0] - half
    up = jnp.pad(up, [(0, tail)] + [(0, 0)] * rest)
    down = jnp.pad(down, [(half, 0)] + [(0, 0)] * rest)
    for j in range(n // 2 - 1, 0, -1):
        up = shift(pick(j) + up, axis, 1)
        down = shift(pick(-j) + down, axis, -1)
    return pick(0) + up + down


def direct_sum(pick, axis):
    n = lax.axis_size(axis)
    total = pick(0)
    got = [shift(pick(j), axis, j) for j in range(1, n)]
    for g in got:
        total = total + g
    return total


def xor_swap(a, axis, bit):
    return lax.ppermute(a, axis, [(i, i ^ bit) for i in range(lax.axis_size(axis))])


def doubled(own, axis):
    n = lax.axis_size(axis)
    at = lax.axis_index(axis)
    got, bit = own[None], n // 2
    while bit:
        other = xor_swap(got, axis, bit)
        low = (at // bit) % 2 == 0
        got = jnp.stack([jnp.where(low, got, other), jnp.where(low, other, got)], 1).reshape(-1, *own.shape)
        bit //= 2
    return got


def ring_pieces(own, axis, half):
    n = lax.axis_size(axis)
    pieces = [(0, 0, own)]
    up = down = own
    for j in range(1, n // 2):
        up = shift(up, axis, 1)
        down = shift(down, axis, -1)
        pieces += [(j, 0, up), (-j, 0, down)]
    pieces += [(n // 2, 0, shift(up[:half], axis, 1)), (n // 2, half, shift(down[half:], axis, -1))]
    return pieces


def shards(
    slope_query,
    slope_key,
    slope_value,
    slope_mixed,
    slope_norm,
    slope_bias,
    param_query,
    param_key,
    param_value,
    param_mixed,
    param_norm,
    param_bias,
    state_query,
    state_key,
    state_value,
    state_mixed,
    state_norm,
    state_bias,
):
    nz, nx = lax.axis_size("z"), lax.axis_size("x")
    iz, ix = lax.axis_index("z"), lax.axis_index("x")
    rows, cols = param_query.shape

    small = jnp.stack([slope_norm[0].reshape(nz, nx, rows), slope_bias[0].reshape(nz, nx, rows)], 2)
    small = small.reshape(nz, nx, 1, 2 * rows)
    small = jnp.pad(small, [(0, 0), (0, 0), (0, 7), (0, cols - 2 * rows)])
    first = [a.reshape(nz, nx, -1, cols) for a in (slope_query, slope_key, small)]
    second = [a.reshape(nz, nx, -1, cols) for a in (slope_value, slope_mixed[0].T)]

    def over_x(j):
        return jnp.concatenate([lax.dynamic_index_in_dim(a, (ix + j) % nx, 1, keepdims=False) for a in first], 1)

    def over_z(j):
        return jnp.concatenate([lax.dynamic_index_in_dim(a, (iz + j) % nz, 0, keepdims=False) for a in second], 1)

    part_first = ring_sum(over_x, "x", nz // 2)
    part_second = ring_sum(over_z, "z", nx // 2)
    first = direct_sum(lambda j: lax.dynamic_index_in_dim(part_first, (iz + j) % nz, 0, keepdims=False), "z")
    second = direct_sum(lambda j: lax.dynamic_index_in_dim(part_second, (ix + j) % nx, 0, keepdims=False), "x")

    mean_rate = (nz * nx) ** (-0.5)
    mean = jnp.concatenate([first[: 2 * rows], second]) * mean_rate
    mean_small = first[2 * rows, : 2 * rows] * mean_rate
    param = jnp.concatenate([param_query, param_key, param_value, param_mixed.T])
    state = jnp.concatenate([state_query, state_key, state_value, state_mixed.T])
    param_small = jnp.concatenate([param_norm, param_bias])
    state_small = jnp.concatenate([state_norm, state_bias])

    own = jnp.sum(param * param, axis=1)
    own = own + shift(own, "tp", 1)
    size = jnp.sum(mean * mean, axis=1)
    size = size + shift(size, "tp", 1)
    mean = mean * (jnp.sqrt(own) * lax.rsqrt(size + 1e-06))[:, None]
    state_new = hold_rate * state + (1.0 - hold_rate) * mean * mean
    following = param - learn_rate * mean * lax.rsqrt(state_new + 1e-06)
    state_new_small = hold_rate * state_small + (1.0 - hold_rate) * mean_small * mean_small
    next_small = param_small - learn_rate * mean_small * lax.rsqrt(state_new_small + 1e-06)

    half = following.astype(jnp.bfloat16)
    half_small = jnp.pad(next_small.astype(jnp.bfloat16)[None], [(0, 7), (0, cols - 2 * rows)])
    first = jnp.concatenate([half[: 2 * rows], half_small])
    second = half[2 * rows :]

    first = doubled(first, "z")
    second = doubled(second, "x")
    half_query = half_key = half_value = half_mixed = jnp.zeros((nz, nx, rows, cols), half.dtype)
    half_small = jnp.zeros((nz, nx, 2 * rows), half.dtype)
    for back, at, piece in ring_pieces(first, "x", nz // 2):
        where = (at, (ix - back) % nx, 0, 0)
        piece = piece[:, None]
        half_query = lax.dynamic_update_slice(half_query, piece[:, :, :rows], where)
        half_key = lax.dynamic_update_slice(half_key, piece[:, :, rows : 2 * rows], where)
        half_small = lax.dynamic_update_slice(half_small, piece[:, :, 2 * rows, : 2 * rows], where[:3])
    for back, at, piece in ring_pieces(second, "z", nx // 2):
        where = ((iz - back) % nz, at, 0, 0)
        piece = piece[None]
        half_value = lax.dynamic_update_slice(half_value, piece[:, :, :rows], where)
        half_mixed = lax.dynamic_update_slice(half_mixed, piece[:, :, rows:], where)

    def whole(a):
        return a.reshape(nz * nx * rows, cols)

    parts = [following[i * rows : (i + 1) * rows] for i in range(4)]
    states = [state_new[i * rows : (i + 1) * rows] for i in range(4)]
    return (
        whole(half_query),
        whole(half_key),
        whole(half_value),
        whole(half_mixed).T,
        half_small[:, :, :rows].reshape(-1),
        half_small[:, :, rows:].reshape(-1),
        parts[0],
        parts[1],
        parts[2],
        parts[3].T,
        next_small[:rows],
        next_small[rows:],
        states[0],
        states[1],
        states[2],
        states[3].T,
        state_new_small[:rows],
        state_new_small[rows:],
    )


def solution(mesh):
    trial, dp, tp = (mesh.shape[a] for a in ("trial", "dp", "tp"))
    fine = Mesh(mesh.devices.reshape(trial, dp // 4, 4, tp), ("trial", "z", "x", "tp"))
    rows = P(("trial", "z", "x"), "tp")
    cols = P(("trial", "tp"), ("z", "x"))
    flat = P(("trial", "z", "x"))
    stack = P(("trial", "z", "x"), None, "tp")
    shares = (rows, rows, rows, cols, flat, flat)
    in_specs = (stack, stack, stack, P(("trial", "z", "x"), "tp", None), P(("trial", "z", "x"), None), P(("trial", "z", "x"), None))
    in_specs = in_specs + shares + shares
    out_specs = (P("trial", "tp"),) * 3 + (P(("trial", "tp"), None), P("trial"), P("trial")) + shares + shares
    return jax.shard_map(shards, mesh=fine, in_specs=in_specs, out_specs=out_specs, check_vma=False)
```

```python
import jax
import jax.numpy as jnp
from jax import lax
from jax.sharding import Mesh
from jax.sharding import PartitionSpec as P

learn_rate = 0.02
hold_rate = 0.8


def swap_xor(a, axis, bits):
    return lax.ppermute(a, axis, [(i, i ^ bits) for i in range(lax.axis_size(axis))])


def swap_near(a, axis):
    return swap_xor(a, axis, 1)


def swap_past(a, axis):
    n = lax.axis_size(axis)
    return lax.ppermute(a, axis, [(i, (i + (1 if i % 2 else -1)) % n) for i in range(n)])


def swap_split(a, axis):
    n = lax.axis_size(axis)
    pairs = []
    for i in range(n):
        pairs.append((2 * i, 2 * (i ^ 1)))
        pairs.append((2 * i + 1, 2 * ((i + (1 if i % 2 else -1)) % n) + 1))
    return lax.ppermute(a, (axis, "tp"), pairs)


def ring_sum(pick, axis):
    n = lax.axis_size(axis)
    even = lax.axis_index(axis) % 2 == 0
    side = jnp.where(even, 1, -1)
    far = pick(n // 2)
    half = far.shape[0] // 2
    low, high = [(0, half)] + [(0, 0)] * (far.ndim - 1), [(half, 0)] + [(0, 0)] * (far.ndim - 1)
    near = swap_near(jnp.where(even, far[:half], far[half:]), axis)
    past = swap_past(jnp.where(even, far[half:], far[:half]), axis)
    near, past = (
        jnp.where(even, jnp.pad(near, high), jnp.pad(near, low)),
        jnp.where(even, jnp.pad(past, low), jnp.pad(past, high)),
    )
    for j in range(n // 2 - 1, 0, -1):
        near, past = (swap_near(pick(side * j) + past, axis), swap_past(pick(-side * j) + near, axis))
    return pick(0) + near + past


def direct_sum(pick, axis):
    n = lax.axis_size(axis)
    at = lax.axis_index(axis)
    total = pick(at)
    for got in [swap_xor(pick(at ^ bits), axis, bits) for bits in range(1, n)]:
        total = total + got
    return total


def paired_sum(part, axis):
    n = lax.axis_size(axis)
    at = lax.axis_index(axis)
    part = part.reshape(n // 2, 2, *part.shape[1:])
    got = swap_split(lax.dynamic_index_in_dim(part, 1 - at % 2, 1, keepdims=False), axis)
    mine = lax.dynamic_index_in_dim(part, at % 2, 1, keepdims=False) + got
    total = lax.dynamic_index_in_dim(mine, at // 2, 0, keepdims=False)
    for bits in range(2, n, 2):
        chunk = lax.dynamic_index_in_dim(mine, (at ^ bits) // 2, 0, keepdims=False)
        total = total + swap_xor(chunk, axis, bits)
    return total


def paired_gather(own, axis):
    n = lax.axis_size(axis)
    at = lax.axis_index(axis)
    mine = jnp.zeros((n // 2, *own.shape), own.dtype)
    for bits in range(0, n, 2):
        piece = swap_xor(own, axis, bits) if bits else own
        mine = lax.dynamic_update_slice(mine, piece[None], ((at ^ bits) // 2, *(0,) * own.ndim))
    other = swap_split(mine, axis)
    odd = at % 2 == 1
    return jnp.stack([jnp.where(odd, other, mine), jnp.where(odd, mine, other)], 1).reshape(n, *own.shape)


def doubled(own, axis):
    n = lax.axis_size(axis)
    at = lax.axis_index(axis)
    got, bit = own[None], n // 2
    while bit:
        other = swap_xor(got, axis, bit)
        low = (at // bit) % 2 == 0
        got = jnp.stack([jnp.where(low, got, other), jnp.where(low, other, got)], 1).reshape(-1, *own.shape)
        bit //= 2
    return got


def ring_pieces(own, axis):
    n = lax.axis_size(axis)
    at = lax.axis_index(axis)
    even = at % 2 == 0
    side = jnp.where(even, 1, -1)
    half = own.shape[0] // 2
    pieces = [(at, 0, own)]
    near = past = own
    for j in range(1, n // 2):
        near, past = swap_near(past, axis), swap_past(near, axis)
        pieces += [((at + side * j) % n, 0, near), ((at - side * j) % n, 0, past)]
    near, past = (
        swap_near(jnp.where(even, past[:half], past[half:]), axis),
        swap_past(jnp.where(even, near[half:], near[:half]), axis),
    )
    far = (at + n // 2) % n
    whole = jnp.where(even, jnp.concatenate([past, near]), jnp.concatenate([near, past]))
    return pieces + [(far, 0, whole)]


def shards(
    slope_query,
    slope_key,
    slope_value,
    slope_mixed,
    slope_norm,
    slope_bias,
    param_query,
    param_key,
    param_value,
    param_mixed,
    param_norm,
    param_bias,
    state_query,
    state_key,
    state_value,
    state_mixed,
    state_norm,
    state_bias,
):
    nz, nx = lax.axis_size("z"), lax.axis_size("x")
    iz, ix = lax.axis_index("z"), lax.axis_index("x")
    rows, cols = param_query.shape

    small = jnp.stack([slope_norm[0].reshape(nz, nx, rows), slope_bias[0].reshape(nz, nx, rows)], 2)
    small = small.reshape(nz, nx, 1, 2 * rows)
    small = jnp.pad(small, [(0, 0), (0, 0), (0, 7), (0, cols - 2 * rows)])
    first = [a.reshape(nz, nx, -1, cols) for a in (slope_query, slope_key, small)]
    second = [a.reshape(nz, nx, -1, cols) for a in (slope_value, slope_mixed[0].T)]

    def over_x(j):
        return jnp.concatenate([lax.dynamic_index_in_dim(a, (ix + j) % nx, 1, keepdims=False) for a in first], 1)

    def over_z(j):
        return jnp.concatenate([lax.dynamic_index_in_dim(a, (iz + j) % nz, 0, keepdims=False) for a in second], 1)

    part_first = ring_sum(over_x, "x")
    part_second = ring_sum(over_z, "z")
    first = paired_sum(part_first, "z")
    second = direct_sum(lambda j: lax.dynamic_index_in_dim(part_second, j, 0, keepdims=False), "x")

    mean_rate = (nz * nx) ** (-0.5)
    mean = jnp.concatenate([first[: 2 * rows], second]) * mean_rate
    mean_small = first[2 * rows, : 2 * rows] * mean_rate
    param = jnp.concatenate([param_query, param_key, param_value, param_mixed.T])
    state = jnp.concatenate([state_query, state_key, state_value, state_mixed.T])
    param_small = jnp.concatenate([param_norm, param_bias])
    state_small = jnp.concatenate([state_norm, state_bias])

    own = jnp.sum(param * param, axis=1)
    own = own + swap_xor(own, "tp", 1)
    size = jnp.sum(mean * mean, axis=1)
    size = size + swap_xor(size, "tp", 1)
    mean = mean * (jnp.sqrt(own) * lax.rsqrt(size + 1e-06))[:, None]
    state_new = hold_rate * state + (1.0 - hold_rate) * mean * mean
    following = param - learn_rate * mean * lax.rsqrt(state_new + 1e-06)
    state_new_small = hold_rate * state_small + (1.0 - hold_rate) * mean_small * mean_small
    next_small = param_small - learn_rate * mean_small * lax.rsqrt(state_new_small + 1e-06)

    half = following.astype(jnp.bfloat16)
    half_small = jnp.pad(next_small.astype(jnp.bfloat16)[None], [(0, 7), (0, cols - 2 * rows)])
    first = jnp.concatenate([half[: 2 * rows], half_small])
    second = half[2 * rows :]

    first = paired_gather(first, "z")
    second = doubled(second, "x")
    half_query = half_key = jnp.zeros((nz, nx, rows, cols), half.dtype)
    half_small = jnp.zeros((nz, nx, 2 * rows), half.dtype)
    for source, at, piece in ring_pieces(first, "x"):
        where = (at, source, 0, 0)
        piece = piece[:, None]
        half_query = lax.dynamic_update_slice(half_query, piece[:, :, :rows], where)
        half_key = lax.dynamic_update_slice(half_key, piece[:, :, rows : 2 * rows], where)
        half_small = lax.dynamic_update_slice(half_small, piece[:, :, 2 * rows, : 2 * rows], where[:3])
    second = paired_gather(second, "z")
    half_value = second[:, :, :rows]
    half_mixed = second[:, :, rows:]

    def whole(a):
        return a.reshape(nz * nx * rows, cols)

    parts = [following[i * rows : (i + 1) * rows] for i in range(4)]
    states = [state_new[i * rows : (i + 1) * rows] for i in range(4)]
    return (
        whole(half_query),
        whole(half_key),
        whole(half_value),
        whole(half_mixed).T,
        half_small[:, :, :rows].reshape(-1),
        half_small[:, :, rows:].reshape(-1),
        parts[0],
        parts[1],
        parts[2],
        parts[3].T,
        next_small[:rows],
        next_small[rows:],
        states[0],
        states[1],
        states[2],
        states[3].T,
        state_new_small[:rows],
        state_new_small[rows:],
    )


def solution(mesh):
    trial, dp, tp = (mesh.shape[a] for a in ("trial", "dp", "tp"))
    fine = Mesh(mesh.devices.reshape(trial, dp // 4, 4, tp), ("trial", "z", "x", "tp"))
    rows = P(("trial", "z", "x"), "tp")
    cols = P(("trial", "tp"), ("z", "x"))
    flat = P(("trial", "z", "x"))
    stack = P(("trial", "z", "x"), None, "tp")
    shares = (rows, rows, rows, cols, flat, flat)
    in_specs = (stack, stack, stack, P(("trial", "z", "x"), "tp", None), P(("trial", "z", "x"), None), P(("trial", "z", "x"), None))
    in_specs = in_specs + shares + shares
    out_specs = (P("trial", "tp"),) * 3 + (P(("trial", "tp"), None), P("trial"), P("trial")) + shares + shares
    return jax.shard_map(shards, mesh=fine, in_specs=in_specs, out_specs=out_specs, check_vma=False)
```
